32 devices in a mesh: tower: 8 (over y, x, core), member: 4 (over z).
Axes of the slice: x: 2, y: 2, z: 4, core: 2. Of those that a mesh axis runs over, the one named last changes fastest.
Arguments:
- slabs: bfloat16 [8, 1024, 4096], P('tower', None, 'member'), may hold values from -6 to 6
- cross_down: bfloat16 [8, 2, 4096, 512], P('tower', None, None, 'member'), may hold values from -0.09375 to 0.09375
- cross_up: bfloat16 [8, 2, 4096, 512], P('tower', None, None, 'member'), may hold values from -0.25 to 0.25
- cross_bias: float32 [8, 2, 4096], P('tower'), may hold values from -3 to 3
- projector: bfloat16 [8, 4096, 2048], P('tower'), may hold values from -0.09375 to 0.09375
- placement: int32 [8, 32], P('tower'), may hold values from 0 to 31, each once within a row
- owner: int32 [4, 256], replicated, may hold values from 0 to 255, each once within a row
- inter_grad: bfloat16 [1024, 16384], P(('tower', 'member')), may hold values from -6 to 6
Outputs:
- interactions: float32 [1024, 16384], P(('tower', 'member'))
- slab_grad: bfloat16 [8, 1024, 4096], P('tower', None, 'member')
The draws below stay inside these ranges and needn't reach their ends.
Inputs may be any that keep to these rules, and one draw needn't show every extreme that they name: Each row of placement names every feature of its tower once. Each row of owner names every sample of its block once.
All inputs are finite; a program needn't handle non-finite values.
Results may differ from the reference program's by a relative error of at most 0.018.
Values may be sent and summed in bfloat16 or wider, within the bound.
No kernel may reach another device: no remote copies, remote signals or barrier semaphores. Data moves between devices by JAX's collectives and lax.ppermute only.
A program may use at most 128 MiB of HBM per device.

```python
import jax
import jax.numpy as jnp
from jax import lax

EMB = 128
FEATS = 32
RANK = 512
VECS = 128
LAYERS = 2
ROWS = 256
WIDTH = 4096
TOWERS = 8
MEMBERS = 4
SAMPLES = 1024
OWNED = 32
TOWER_OUT = 2048


def block_scale(stream_key, dims, split, smallest, high):
    def one(dim, parts):
        heights = jax.random.uniform(jax.random.fold_in(jax.random.fold_in(stream_key, 6), dim), (parts,), jnp.float32, smallest / len(split), high / len(split))
        return jnp.repeat(jnp.exp(heights), dims[dim] // parts).reshape((-1,) + (1,) * (len(dims) - dim - 1))

    loudness = one(*split[0])
    for cut in split[1:]:
        loudness = loudness * one(*cut)
    return loudness


def scatter_about(own_key, dims, deviation, limit, split=(), kind=jnp.bfloat16):
    factor_of = block_scale(own_key, dims, split, -0.22, 0.18) if split else 1.0
    drawn = jax.random.normal(own_key, dims, jnp.float32) * deviation * factor_of
    return jnp.minimum(jnp.maximum(drawn, -limit), limit).astype(kind)


def setup_inputs(seed: int = 0) -> dict:
    seeds = jax.random.split(jax.random.key(seed), 9)
    return {
        "slabs": scatter_about(seeds[0], (TOWERS, SAMPLES, WIDTH), 1.0, 6.0, ((0, 8), (2, 4))),
        "cross_down": scatter_about(seeds[1], (TOWERS, LAYERS, WIDTH, RANK), WIDTH ** -0.5, 0.09375, ((0, 8), (3, 4))),
        "cross_up": scatter_about(seeds[2], (TOWERS, LAYERS, WIDTH, RANK), RANK ** -0.5, 0.25, ((0, 8), (3, 4))),
        "cross_bias": scatter_about(seeds[3], (TOWERS, LAYERS, WIDTH), 0.5, 3.0, ((0, 8),), jnp.float32),
        "projector": scatter_about(seeds[4], (TOWERS, WIDTH, TOWER_OUT), WIDTH ** -0.5, 0.09375, ((0, 8),)),
        "placement": jax.vmap(lambda own: jax.random.permutation(own, FEATS))(jax.random.split(seeds[5], TOWERS)).reshape((TOWERS, FEATS)).astype(jnp.int32),
        "owner": jax.vmap(lambda own: jax.random.permutation(own, ROWS))(jax.random.split(seeds[6], MEMBERS)).reshape((MEMBERS, ROWS)).astype(jnp.int32),
        "inter_grad": scatter_about(seeds[7], (SAMPLES, VECS * VECS), 1.0, 6.0, ((0, 32),)),
    }


def tower_forward(inputs, downs, ups, biases, projection):
    current = inputs
    start_f = inputs.astype(jnp.float32)
    scales = []
    for depth in range(LAYERS):
        hidden = jnp.dot(current, downs[depth], preferred_element_type=jnp.float32).astype(jnp.bfloat16)
        scale_now = jnp.dot(hidden, ups[depth].T, preferred_element_type=jnp.float32) + biases[depth]
        scales.append(scale_now)
        current = (start_f * scale_now + current.astype(jnp.float32)).astype(jnp.bfloat16)
    vector = jnp.dot(current, projection, preferred_element_type=jnp.float32).astype(jnp.bfloat16)
    return vector, scales


def placed(slab, order):
    return slab.reshape(SAMPLES, FEATS, EMB)[:, order].reshape(SAMPLES, WIDTH)


def reference(slabs, cross_down, cross_up, cross_bias, projector, placement, owner, inter_grad):
    def forward_one(items):
        slab, downs, ups, biases, projection, order = items
        vector, scales = tower_forward(placed(slab, order), downs, ups, biases, projection)
        return vector

    vectors = lax.map(forward_one, (slabs, cross_down, cross_up, cross_bias, projector, placement))
    per_sample = jnp.transpose(vectors, (1, 0, 2)).reshape(SAMPLES, VECS, EMB).astype(jnp.float32)
    table = jnp.einsum('bie,bje->bij', per_sample, per_sample) / EMB
    position = jnp.arange(SAMPLES, dtype=jnp.int32)
    block = position // OWNED
    tower_of = block // MEMBERS
    member_of = block % MEMBERS
    local = tower_of * OWNED + position % OWNED
    index = (member_of * ROWS + owner[member_of, local]).astype(jnp.int32)
    interactions = table.reshape(SAMPLES, VECS * VECS)[index]
    cotangent = jnp.zeros((SAMPLES, VECS * VECS), jnp.float32).at[index].set(inter_grad.astype(jnp.float32))
    cotangent = cotangent.reshape(SAMPLES, VECS, VECS)
    symmetric = cotangent + jnp.swapaxes(cotangent, 1, 2)
    vec_grad = (jnp.einsum('bij,bje->bie', symmetric, per_sample) / EMB).astype(jnp.bfloat16)
    per_tower = jnp.transpose(vec_grad.reshape(SAMPLES, TOWERS, TOWER_OUT), (1, 0, 2))

    def backward_one(items):
        slab, downs, ups, biases, projection, order, vector_grad = items
        inputs = placed(slab, order)
        vector, scales = tower_forward(inputs, downs, ups, biases, projection)
        inputs_f = inputs.astype(jnp.float32)
        gradient = jnp.dot(vector_grad, projection.T, preferred_element_type=jnp.float32)
        accum = jnp.zeros((SAMPLES, WIDTH), jnp.float32)
        for depth in reversed(range(LAYERS)):
            accum = accum + gradient * scales[depth]
            dscale = (gradient * inputs_f).astype(jnp.bfloat16)
            dhidden = jnp.dot(dscale, ups[depth], preferred_element_type=jnp.float32).astype(jnp.bfloat16)
            gradient = gradient + jnp.dot(dhidden, downs[depth].T, preferred_element_type=jnp.float32)
        total = (gradient + accum).astype(jnp.bfloat16)
        inverse = jnp.argsort(order).astype(jnp.int32)
        return total.reshape(SAMPLES, FEATS, EMB)[:, inverse].reshape(SAMPLES, WIDTH)

    slab_grad = lax.map(backward_one, (slabs, cross_down, cross_up, cross_bias, projector, placement, per_tower))
    return interactions, slab_grad
```

```python
import jax
import jax.numpy as jnp
from jax import lax
from jax.sharding import PartitionSpec as P

AXES = ("tower", "member")


def make_step(tower_n, member_n):
    half = member_n // 2

    def device(t, m):
        return t * member_n + m

    devices = [(t, m) for t in range(tower_n) for m in range(member_n)]

    def computes(t, m, block):
        return device(t - t % 2 + block // half, (t % 2) * half + block % half)

    spread = [
        [(device(t, m), computes(t, m, m ^ k)) for t, m in devices] for k in range(member_n)
    ]
    collect = [[(b, a) for a, b in pairs] for pairs in spread]
    swap = spread[0]
    near = [(device(t, m), device(t, m ^ 1)) for t, m in devices]
    core = [(device(t, m), device(t ^ 1, m)) for t, m in devices]
    lend = [
        (device(t, m), device(t ^ 1, m)) for t, m in devices if t % 2 == m // half
    ]

    def send(value, pairs):
        return lax.ppermute(value, AXES, pairs)

    def gather_map(shard):
        own = send(shard, swap)
        side = send(own, near)
        return jnp.concatenate([own, side, send(own, core), send(side, core)], axis=-1)

    def per_device(slabs, cross_down, cross_up, cross_bias, projector, placement, owner, inter_grad):
        tower = lax.axis_index("tower")
        member = lax.axis_index("member")
        block = (tower % 2) * half + member % half
        at_home = tower % 2 == member // half
        depth_count = cross_down.shape[1]
        features = placement.shape[1]
        local_features = features // member_n
        row_count = slabs.shape[1] // member_n
        local_width = slabs.shape[2]
        full_width = local_width * member_n
        slot_width = full_width // features

        def borrowed(value):
            return jnp.where(at_home, value, send(value, lend))

        order = borrowed(placement)[0]
        biases = borrowed(cross_bias)[0]
        project = borrowed(projector)[0]

        by_block = slabs[0].reshape(member_n, row_count, local_width)
        pieces = [
            send(lax.dynamic_index_in_dim(by_block, member ^ k, 0, keepdims=False), spread[k])
            for k in range(member_n)
        ]
        downs, ups = [], []
        for depth in range(depth_count):
            downs.append(gather_map(cross_down[0, depth]))
            ups.append(gather_map(cross_up[0, depth]))

        own_row = lax.dynamic_index_in_dim(owner, block, 0, keepdims=False)
        inverse_own = jnp.argsort(own_row)
        inverse_place = jnp.argsort(order)
        position = ((order // local_features) ^ block) * local_features + order % local_features
        inputs = (
            jnp.concatenate(pieces, axis=1)[own_row]
            .reshape(row_count, features, slot_width)[:, position]
            .reshape(row_count, full_width)
        )
        inputs_f = inputs.astype(jnp.float32)
        current = inputs
        scales = []
        for depth in range(depth_count):
            hidden = jnp.dot(current, downs[depth], preferred_element_type=jnp.float32).astype(
                jnp.bfloat16
            )
            scale_now = (
                jnp.dot(hidden, ups[depth].T, preferred_element_type=jnp.float32) + biases[depth]
            )
            scales.append(scale_now)
            current = (inputs_f * scale_now + current.astype(jnp.float32)).astype(jnp.bfloat16)
        vector = jnp.dot(current, project, preferred_element_type=jnp.float32).astype(jnp.bfloat16)

        per_tower = vector.shape[1] // slot_width
        vector_count = per_tower * tower_n
        owned_rows = row_count // tower_n
        vector = send(vector.reshape(tower_n, owned_rows, per_tower, slot_width), swap)
        owned = lax.all_to_all(vector, "tower", split_axis=0, concat_axis=0, tiled=True)
        owned = jnp.swapaxes(owned, 0, 1).reshape(owned_rows, vector_count, slot_width)
        table = (
            jnp.einsum("bie,bje->bij", owned, owned, preferred_element_type=jnp.float32)
            / slot_width
        )
        interactions = table.reshape(owned_rows, vector_count * vector_count)
        cotangent = inter_grad.astype(jnp.float32).reshape(owned_rows, vector_count, vector_count)
        symmetric = (cotangent + jnp.swapaxes(cotangent, 1, 2)).astype(jnp.bfloat16)
        vec_grad = (
            jnp.einsum("bij,bje->bie", symmetric, owned, preferred_element_type=jnp.float32)
            / slot_width
        ).astype(jnp.bfloat16)
        vec_grad = jnp.swapaxes(
            vec_grad.reshape(owned_rows, tower_n, per_tower, slot_width), 0, 1
        )
        returned = lax.all_to_all(vec_grad, "tower", split_axis=0, concat_axis=0, tiled=True)
        local_grad = send(returned, swap).reshape(row_count, per_tower * slot_width)

        gradient = jnp.dot(local_grad, project.T, preferred_element_type=jnp.float32)
        accum = jnp.zeros((row_count, full_width), jnp.float32)
        for depth in reversed(range(depth_count)):
            accum = accum + gradient * scales[depth]
            dscale = (gradient * inputs_f).astype(jnp.bfloat16)
            dhidden = jnp.dot(dscale, ups[depth], preferred_element_type=jnp.float32).astype(
                jnp.bfloat16
            )
            gradient = gradient + jnp.dot(
                dhidden, downs[depth].T, preferred_element_type=jnp.float32
            )
        total = (gradient + accum).astype(jnp.bfloat16)
        total = total[inverse_own].reshape(row_count, features, slot_width)
        slab_grad = jnp.zeros((member_n, row_count, local_width), jnp.bfloat16)
        for k in range(member_n):
            slots = lax.dynamic_slice_in_dim(
                inverse_place, (block ^ k) * local_features, local_features
            )
            piece = send(total[:, slots].reshape(row_count, local_width), collect[k])
            slab_grad = lax.dynamic_update_index_in_dim(slab_grad, piece, member ^ k, 0)
        return (interactions, slab_grad.reshape(1, member_n * row_count, local_width))

    return per_device


def solution(mesh):
    placed = (
        P("tower", None, "member"),
        P("tower", None, None, "member"),
        P("tower", None, None, "member"),
        P("tower", None, None),
        P("tower", None, None),
        P("tower", None),
        P(),
        P(("tower", "member"), None),
    )
    return jax.shard_map(
        make_step(mesh.shape["tower"], mesh.shape["member"]),
        mesh=mesh,
        in_specs=placed,
        out_specs=(P(("tower", "member"), None), P("tower", None, "member")),
        check_vma=False,
    )
```
